32 devices in a mesh: dp: 4 (over y, core), seq: 2 (over x), expert: 4 (over z).
Axes of the slice: x: 2, y: 2, z: 4, core: 2. Of those that a mesh axis runs over, the one named last changes fastest.
Arguments:
- queries: bfloat16 [16, 256, 2560], P(('dp', 'expert'), 'seq'), may hold values from -100 to 100
- key_rows: bfloat16 [16, 256, 512], P(('dp', 'expert'), 'seq'), may hold values from -5 to 5
- value_entries: bfloat16 [16, 256, 512], P(('dp', 'expert'), 'seq'), may hold values from -6 to 6
- features: bfloat16 [4096, 2560], P(('dp', 'seq', 'expert')), may hold values from -0.29882812 to 0.29882812
- router_score: float32 [4096], P(('dp', 'seq', 'expert')), may hold values from -8 to 8
- expert_index: int32 [4096], P(('dp', 'seq', 'expert')), may hold values from 0 to 31, as said below
- slot_index: int32 [4096], P(('dp', 'seq', 'expert')), may hold values from 0 to 35, as said below
- expert_grad: bfloat16 [4608, 2560], P(('dp', 'seq', 'expert')), may hold values from -12 to 12
Outputs:
- attention: bfloat16 [16, 256, 2560], P(('dp', 'expert'), 'seq')
- input_grad: bfloat16 [4096, 2560], P(('dp', 'seq', 'expert'))
- score_grad: float32 [4096], P(('dp', 'seq', 'expert'))
- router_grad: float32 [32, 2560], P('expert', ('dp', 'seq'))
The draws below stay inside these ranges and needn't reach their ends.
Inputs may be any that keep to these rules, and one draw needn't show every extreme that they name: Among the 128 tokens of one device (aligned blocks, devices in the order dp, seq, expert), at most 36 have one value of expert_index // 8; in every draw some value takes exactly 36 tokens in every block. Tokens of one block with the same expert_index // 8 have different slot_index.
All inputs are finite; a program needn't handle non-finite values.
Results may differ from the reference program's by a relative error of at most 0.0046.
Values may be sent and summed in bfloat16 or wider, within the bound.
No kernel may reach another device: no remote copies, remote signals or barrier semaphores. Data moves between devices by JAX's collectives and lax.ppermute only.
A program may use at most 64 MiB of HBM per device.

```python
import math
import jax
import jax.numpy as jnp
from jax import lax

QUERY_HEADS = 20
KEY_VALUE_HEADS = 4
HEAD_SIZE = 128
DW = 2560
EXP_DEV = 8
TOK_DEV = 128
EXPERTS = 32
CAP = 36
SEQUENCE_LENGTH = 256
SEQUENCE_COUNT = 16
TOKENS = 4096
SLOTS = 4608
N_EXPERT = 4


def drawn_keys(key):
    starting_keys = jnp.clip(jax.random.normal(jax.random.fold_in(key, 31), (SEQUENCE_COUNT, SEQUENCE_LENGTH, KEY_VALUE_HEADS * HEAD_SIZE), jnp.float32), -5.0, 5.0)
    return starting_keys


def draw_key_rows(key, part):
    return drawn_keys(key).astype(jnp.bfloat16)


def draw_queries(key, part):
    base_query = jnp.clip(jax.random.normal(jax.random.fold_in(key, 37), (SEQUENCE_COUNT, SEQUENCE_LENGTH, QUERY_HEADS * HEAD_SIZE), jnp.float32), -5.0, 5.0)
    return base_query.astype(jnp.bfloat16)


def route_cells(key):
    block_count = TOKENS // TOK_DEV
    cell_total = N_EXPERT * CAP
    everyone = jax.random.randint(jax.random.fold_in(key, 41), (), 0, N_EXPERT)
    block_keys = jax.random.split(jax.random.fold_in(key, 43), block_count)

    def one_block(block_key):
        first_key, second_key, third_key, fourth_key = jax.random.split(block_key, 4)
        extra_full = jax.random.randint(first_key, (), 0, N_EXPERT)
        cell_ids = jnp.arange(cell_total, dtype=jnp.int32)
        target = cell_ids // CAP
        noise_bits = jax.random.randint(second_key, (cell_total,), 0, 2 ** 18)
        forced = (target == everyone) | (target == extra_full)
        cell_score = jnp.where(forced, cell_ids, (noise_bits + 1) * 4096 + cell_ids)
        cell_order = jnp.argsort(cell_score, stable=True).astype(jnp.int32)
        chosen = cell_order[:TOK_DEV]
        shuffled = chosen[jax.random.permutation(third_key, TOK_DEV)]
        local_pick = jax.random.randint(fourth_key, (TOK_DEV,), 0, EXP_DEV)
        return (shuffled // CAP * EXP_DEV + local_pick, shuffled % CAP)
    index_all, slot_all = jax.vmap(one_block)(block_keys)
    return (index_all.reshape(TOKENS).astype(jnp.int32), slot_all.reshape(TOKENS).astype(jnp.int32))


def draw_expert_index(key, part):
    return route_cells(key)[0]


def draw_slot_index(key, part):
    return route_cells(key)[1]


def steps_of(own_key, dims, cuts, smallest, high):
    level = 1.0
    for position, parts in cuts:
        steps = jax.random.uniform(jax.random.fold_in(jax.random.fold_in(own_key, 6), position), (parts,), jnp.float32, smallest / len(cuts), high / len(cuts))
        level = level * jnp.repeat(jnp.exp(steps), dims[position] // parts).reshape((-1,) + (1,) * (len(dims) - 1 - position))
    return level


def scatter_about(key, shape, spread, limit, cuts=(), kind=jnp.bfloat16):
    gain = steps_of(key, shape, cuts, -0.22, 0.18) if cuts else 1.0
    result = jax.random.normal(key, shape, jnp.float32) * spread * gain
    return jnp.minimum(jnp.maximum(result, -limit), limit).astype(kind)


def setup_inputs(seed: int = 0) -> dict:
    arg_keys = jax.random.split(jax.random.key(seed), 9)
    return {
        "queries": draw_queries(jax.random.fold_in(arg_keys[8], 71), 0),
        "key_rows": draw_key_rows(jax.random.fold_in(arg_keys[8], 71), 0),
        "value_entries": scatter_about(arg_keys[2], (SEQUENCE_COUNT, SEQUENCE_LENGTH, KEY_VALUE_HEADS * HEAD_SIZE), 1.0, 6.0, ((0, 16), (1, 2))),
        "features": scatter_about(arg_keys[3], (TOKENS, DW), 0.05, 0.29882812, ((0, 32),)),
        "router_score": scatter_about(arg_keys[4], (TOKENS,), 2.0, 8.0, ((0, 32),), jnp.float32),
        "expert_index": draw_expert_index(jax.random.fold_in(arg_keys[8], 71), 0),
        "slot_index": draw_slot_index(jax.random.fold_in(arg_keys[8], 71), 0),
        "expert_grad": scatter_about(arg_keys[7], (SLOTS, DW), 2.0, 12.0, ((0, 32),)),
    }


def attend_sequence(query_sequence, key_sequence, value_sequence):
    group_width = QUERY_HEADS // KEY_VALUE_HEADS
    query_tiles = query_sequence.reshape(SEQUENCE_LENGTH, KEY_VALUE_HEADS, group_width, HEAD_SIZE).astype(jnp.float32)
    key_tiles = key_sequence.reshape(SEQUENCE_LENGTH, KEY_VALUE_HEADS, HEAD_SIZE).astype(jnp.float32)
    value_tiles = value_sequence.reshape(SEQUENCE_LENGTH, KEY_VALUE_HEADS, HEAD_SIZE).astype(jnp.float32)
    scores = jnp.einsum('qkgd,pkd->kgqp', query_tiles, key_tiles) * (1.0 / math.sqrt(HEAD_SIZE))
    query_pos = lax.broadcasted_iota(jnp.int32, (SEQUENCE_LENGTH, SEQUENCE_LENGTH), 0)
    key_pos = lax.broadcasted_iota(jnp.int32, (SEQUENCE_LENGTH, SEQUENCE_LENGTH), 1)
    scores = jnp.where(query_pos >= key_pos, scores, -jnp.inf)
    row_max = lax.optimization_barrier(jnp.max(scores, axis=-1, keepdims=True))
    exp_scores = jnp.exp(scores - row_max)
    weights = (exp_scores / lax.optimization_barrier(jnp.sum(exp_scores, axis=-1, keepdims=True))).astype(jnp.bfloat16)
    mixed_out = jnp.einsum('kgqp,pkd->qkgd', weights.astype(jnp.float32), value_tiles)
    return mixed_out.reshape(SEQUENCE_LENGTH, QUERY_HEADS * HEAD_SIZE).astype(jnp.bfloat16)

def reference(queries, key_rows, value_entries, features, router_score, expert_index, slot_index, expert_grad):
    attention = lax.map(lambda triple: attend_sequence(triple[0], triple[1], triple[2]), (queries, key_rows, value_entries))
    block_count = TOKENS // TOK_DEV
    device_ids = jnp.arange(block_count, dtype=jnp.int32)

    def one_block(running, inputs):
        feature_block, score_block, index_block, slot_block, device_id = inputs
        home_index = device_id % N_EXPERT
        group_index = device_id // N_EXPERT
        dest_index = index_block // EXP_DEV
        row_ids = (((group_index * N_EXPERT + dest_index) * N_EXPERT + home_index) * CAP + slot_block).astype(jnp.int32)
        routed = jnp.take(expert_grad, row_ids, axis=0).astype(jnp.float32)
        gate_value = jax.nn.sigmoid(score_block)
        input_block = (gate_value[:, None] * routed).astype(jnp.bfloat16)
        feature_wide = feature_block.astype(jnp.float32)
        inner_sum = lax.optimization_barrier(jnp.sum(routed * feature_wide, axis=1))
        grad_block = inner_sum * gate_value * (1.0 - gate_value)
        columns = lax.broadcasted_iota(jnp.int32, (TOK_DEV, EXPERTS), 1)
        weighted = jnp.where(index_block[:, None] == columns, grad_block[:, None], jnp.zeros((), jnp.float32))
        running = running + jnp.dot(weighted.T, feature_wide, precision=lax.Precision.HIGHEST)
        return (running, (input_block, grad_block))
    start_sum = jnp.zeros((EXPERTS, DW), jnp.float32)
    inputs = (features.reshape(block_count, TOK_DEV, DW), router_score.reshape(block_count, TOK_DEV), expert_index.reshape(block_count, TOK_DEV), slot_index.reshape(block_count, TOK_DEV), device_ids)
    router_grad, (input_grad, score_grad) = lax.scan(one_block, start_sum, inputs)
    return (attention, input_grad.reshape(TOKENS, DW), score_grad.reshape(TOKENS), router_grad)
```

```python
import functools
import math

import jax
import jax.numpy as jnp
from jax import lax
from jax.experimental import pallas as pl
from jax.experimental.pallas import tpu as pltpu
from jax.sharding import PartitionSpec as P

HEAD_SIZE = 128
EXP_DEV = 8
DIRECT_LIMIT = 64


def round_up(value, step):
    return (value + step - 1) // step * step


def is_power(value):
    return value & (value - 1) == 0


def partner_pairs(count, step):
    if is_power(count):
        return [(i, i ^ step) for i in range(count)]
    return [(i, (i + step) % count) for i in range(count)]


def block_to_send(me, count, step):
    return me ^ step if is_power(count) else lax.rem(me + step, count)


def source_step(me, count, source):
    if is_power(count):
        return me ^ source
    return lax.rem(me - source + count, count)


def whole_vmem():
    return pl.BlockSpec(memory_space=pltpu.VMEM)


def attention_kernel(seq_count, q_ref, *refs):
    kv_refs, out_ref = refs[:-1], refs[-1]
    head_group = q_ref.shape[2] // HEAD_SIZE
    rows = q_ref.shape[1]
    me = lax.axis_index("seq")
    scale = 1.0 / math.sqrt(HEAD_SIZE)
    lower = lax.broadcasted_iota(jnp.int32, (rows, rows), 0) >= lax.broadcasted_iota(
        jnp.int32, (rows, rows), 1
    )
    keys = [kv_refs[2 * b] for b in range(seq_count)]
    values = [kv_refs[2 * b + 1] for b in range(seq_count)]
    for head in range(head_group):
        span = slice(head * HEAD_SIZE, (head + 1) * HEAD_SIZE)
        query = q_ref[0, :, span]
        tiles = []
        for b in range(seq_count):
            tile = (
                lax.dot_general(
                    query,
                    keys[b][0],
                    (((1,), (1,)), ((), ())),
                    preferred_element_type=jnp.float32,
                )
                * scale
            )
            if b == 0:
                tile = jnp.where(lower, tile, -jnp.inf)
            else:
                tile = jnp.where(lax.rem(me + seq_count - b, seq_count) < me, tile, -jnp.inf)
            tiles.append(tile)
        top = jnp.max(functools.reduce(jnp.maximum, tiles), axis=1, keepdims=True)
        weights = [jnp.exp(tile - top) for tile in tiles]
        total = jnp.sum(functools.reduce(jnp.add, weights), axis=1, keepdims=True)
        mixed = None
        for b in range(seq_count):
            term = jnp.dot(
                weights[b].astype(jnp.bfloat16), values[b][0], preferred_element_type=jnp.float32
            )
            mixed = term if mixed is None else mixed + term
        out_ref[0, :, span] = (mixed / total).astype(jnp.bfloat16)


def attend(queries, key_rows, value_entries):
    seq_count = lax.axis_size("seq")
    batch, rows, width = queries.shape
    kv_heads = key_rows.shape[2] // HEAD_SIZE
    group_columns = width // kv_heads
    key_value = jnp.concatenate([key_rows, value_entries], axis=2)
    operands = [key_rows, value_entries]
    kv_block = (1, rows, HEAD_SIZE)
    specs = [pl.BlockSpec(kv_block, lambda s, h: (s, 0, h))] * 2
    for step in range(1, seq_count):
        pairs = [(i, (i + step) % seq_count) for i in range(seq_count)]
        other = lax.ppermute(key_value, "seq", pairs)
        operands += [other, other]
        specs += [
            pl.BlockSpec(kv_block, lambda s, h: (s, 0, h)),
            pl.BlockSpec(kv_block, lambda s, h: (s, 0, kv_heads + h)),
        ]
    q_spec = pl.BlockSpec((1, rows, group_columns), lambda s, h: (s, 0, h))
    return pl.pallas_call(
        functools.partial(attention_kernel, seq_count),
        grid=(batch, kv_heads),
        in_specs=[q_spec] + specs,
        out_specs=q_spec,
        out_shape=jax.ShapeDtypeStruct(queries.shape, jnp.bfloat16),
        compiler_params=pltpu.CompilerParams(vmem_limit_bytes=16 * 2**20),
        cost_estimate=pl.CostEstimate(
            flops=4 * batch * rows * rows * seq_count * width,
            bytes_accessed=4 * batch * rows * width,
            transcendentals=batch * rows * rows * seq_count * width // HEAD_SIZE,
        ),
        name="attend",
    )(queries, *operands)


def token_cells(count, padded, expert_row, slot_row):
    me = lax.axis_index("expert")
    target = lax.shift_right_logical(expert_row, EXP_DEV.bit_length() - 1)
    return source_step(me, count, target) * padded + slot_row


def slot_kernel(count, padded, expert_ref, slot_ref, score_ref, feature_ref, moved_ref, weight_ref):
    tokens = feature_ref.shape[0]
    cells, experts = weight_ref.shape
    cell_row = token_cells(count, padded, expert_ref[...], slot_ref[...])
    chosen = lax.broadcasted_iota(jnp.int32, (cells, tokens), 0) == cell_row
    gate = 1.0 / (1.0 + jnp.exp(-score_ref[...]))
    slope = jnp.sum(jnp.where(chosen, gate * (1.0 - gate), 0.0), axis=1, keepdims=True)
    owner = jnp.sum(
        jnp.where(chosen, expert_ref[...].astype(jnp.float32), 0.0), axis=1, keepdims=True
    )
    columns = lax.broadcasted_iota(jnp.int32, (cells, experts), 1).astype(jnp.float32)
    weight_ref[...] = jnp.where(owner == columns, slope, 0.0)
    picker = jnp.where(chosen, 1.0, 0.0).astype(jnp.bfloat16)
    moved_ref[...] = jnp.dot(
        picker, feature_ref[...], preferred_element_type=jnp.float32
    ).astype(jnp.bfloat16)


def partial_kernel(count, padded, slab, *refs):
    chunk_refs = refs[:count]
    moved_ref, weight_ref, out_ref, inner_ref = refs[count:]
    cells, experts = weight_ref.shape
    capacity, width = chunk_refs[0].shape
    inner_ref[...] = jnp.zeros_like(inner_ref)
    for k in range(count):
        span = slice(k * padded, k * padded + capacity)
        inner_ref[span, :] = jnp.sum(
            chunk_refs[k][...].astype(jnp.float32) * moved_ref[span, :].astype(jnp.float32),
            axis=1,
            keepdims=True,
        )
    weighted = weight_ref[...] * inner_ref[...]
    high = weighted.astype(jnp.bfloat16)
    low = (weighted - high.astype(jnp.float32)).astype(jnp.bfloat16)
    both = lax.dot_general(
        jnp.concatenate([high, low], axis=1),
        moved_ref[...],
        (((0,), (0,)), ((), ())),
        preferred_element_type=jnp.float32,
    )
    sums = both[:experts] + both[experts:]
    if slab is None:
        out_ref[...] = sums
        return
    rolled = pltpu.roll(sums, width - slab % HEAD_SIZE, 1) if slab % HEAD_SIZE else sums
    groups = experts // EXP_DEV
    for c in range(width // slab):
        start = c * slab
        source = sums
        if start % HEAD_SIZE:
            source, start = rolled, start - slab % HEAD_SIZE
        for e in range(groups):
            out_ref[c * groups + e] = source[
                e * EXP_DEV : (e + 1) * EXP_DEV, start : start + slab
            ].astype(jnp.bfloat16)


def output_kernel(count, padded, expert_ref, slot_ref, score_ref, inner_ref, *refs):
    chunk_refs = refs[:count]
    input_ref, score_out_ref = refs[count:]
    tokens = input_ref.shape[0]
    capacity = chunk_refs[0].shape[0]
    cells = inner_ref.shape[0]
    cell_row = token_cells(count, padded, expert_ref[...], slot_ref[...])
    chosen = lax.broadcasted_iota(jnp.int32, (cells, tokens), 0) == cell_row
    gate = 1.0 / (1.0 + jnp.exp(-score_ref[...]))
    inner = jnp.sum(jnp.where(chosen, inner_ref[...], 0.0), axis=0, keepdims=True)
    score_out_ref[...] = inner * gate * (1.0 - gate)
    square = lax.broadcasted_iota(jnp.int32, (tokens, tokens), 0) == lax.broadcasted_iota(
        jnp.int32, (tokens, tokens), 1
    )
    gate_column = jnp.sum(jnp.where(square, gate, 0.0), axis=1, keepdims=True)
    picker = jnp.where(chosen, 1.0, 0.0)
    routed = None
    for k in range(count):
        part = picker[k * padded : k * padded + capacity].astype(jnp.bfloat16)
        term = lax.dot_general(
            part, chunk_refs[k][...], (((0,), (0,)), ((), ())), preferred_element_type=jnp.float32
        )
        routed = term if routed is None else routed + term
    input_ref[...] = (gate_column * routed).astype(jnp.bfloat16)


def local(
    queries, key_rows, value_entries, features, router_score, expert_index, slot_index, expert_grad
):
    count = lax.axis_size("expert")
    me = lax.axis_index("expert")
    slabs = lax.axis_size("dp") * lax.axis_size("seq")
    capacity = expert_grad.shape[0] // count
    padded = round_up(capacity, 8)
    tokens, width = features.shape
    experts = EXP_DEV * count
    cells = count * padded
    blocks = expert_grad.reshape(count, capacity, width)

    chunks = [lax.dynamic_index_in_dim(blocks, me, 0, keepdims=False)] + [None] * (count - 1)
    for step in range(count - 1, 0, -1):
        piece = lax.dynamic_index_in_dim(
            blocks, block_to_send(me, count, step), 0, keepdims=False
        )
        chunks[step] = lax.ppermute(piece, "expert", partner_pairs(count, step))

    attention = attend(queries, key_rows, value_entries)

    expert_row = expert_index.reshape(1, tokens)
    slot_row = slot_index.reshape(1, tokens)
    score_row = router_score.reshape(1, tokens)
    small = pltpu.CompilerParams(vmem_limit_bytes=16 * 2**20)
    moved, weight = pl.pallas_call(
        functools.partial(slot_kernel, count, padded),
        in_specs=[whole_vmem()] * 4,
        out_specs=[whole_vmem()] * 2,
        out_shape=[
            jax.ShapeDtypeStruct((cells, width), jnp.bfloat16),
            jax.ShapeDtypeStruct((cells, experts), jnp.float32),
        ],
        compiler_params=small,
        cost_estimate=pl.CostEstimate(
            flops=2 * cells * tokens * width, bytes_accessed=4 * tokens * width, transcendentals=0
        ),
        name="to_slots",
    )(expert_row, slot_row, score_row, features)

    slab = width // slabs
    direct = slabs * count <= DIRECT_LIMIT and slab % (HEAD_SIZE // 2) == 0
    sums_shape = (
        jax.ShapeDtypeStruct((slabs * count, EXP_DEV, slab), jnp.bfloat16)
        if direct
        else jax.ShapeDtypeStruct((experts, width), jnp.float32)
    )
    sums, inner = pl.pallas_call(
        functools.partial(partial_kernel, count, padded, slab if direct else None),
        in_specs=[whole_vmem()] * (count + 2),
        out_specs=[whole_vmem()] * 2,
        out_shape=[sums_shape, jax.ShapeDtypeStruct((cells, 1), jnp.float32)],
        compiler_params=small,
        cost_estimate=pl.CostEstimate(
            flops=4 * cells * experts * width, bytes_accessed=2 * cells * width, transcendentals=0
        ),
        name="partial_sums",
    )(*chunks, moved, weight)
    if direct:
        parts = lax.all_to_all(
            sums, ("dp", "seq", "expert"), split_axis=0, concat_axis=0, tiled=True
        )
        router_grad = jnp.sum(parts.astype(jnp.float32), axis=0)
    else:
        per_expert = lax.psum_scatter(sums, "expert", scatter_dimension=0, tiled=True)
        router_grad = lax.psum_scatter(per_expert, ("dp", "seq"), scatter_dimension=1, tiled=True)

    input_grad, score_grad = pl.pallas_call(
        functools.partial(output_kernel, count, padded),
        in_specs=[whole_vmem()] * (count + 4),
        out_specs=[whole_vmem()] * 2,
        out_shape=[
            jax.ShapeDtypeStruct((tokens, width), jnp.bfloat16),
            jax.ShapeDtypeStruct((1, tokens), jnp.float32),
        ],
        compiler_params=small,
        cost_estimate=pl.CostEstimate(
            flops=2 * cells * tokens * width, bytes_accessed=4 * tokens * width, transcendentals=0
        ),
        name="token_outputs",
    )(expert_row, slot_row, score_row, inner, *chunks)
    return (attention, input_grad, score_grad.reshape(tokens), router_grad)


def solution(mesh):
    tokens_spec = P(("dp", "seq", "expert"))
    rows_spec = P(("dp", "seq", "expert"), None)
    sequence_spec = P(("dp", "expert"), "seq", None)
    return jax.shard_map(
        local,
        mesh=mesh,
        in_specs=(
            sequence_spec,
            sequence_spec,
            sequence_spec,
            rows_spec,
            tokens_spec,
            tokens_spec,
            tokens_spec,
            rows_spec,
        ),
        out_specs=(sequence_spec, rows_spec, tokens_spec, P("expert", ("dp", "seq"))),
        check_vma=False,
    )
```
